32 devices in a mesh: gx: 2 (over y), gy: 4 (over x, core), gz: 4 (over z).
Axes of the slice: x: 2, y: 2, z: 4, core: 2. Of those that a mesh axis runs over, the one named last changes fastest.
Arguments:
- gradients: bfloat16 [32, 851968], P(('gx', 'gy', 'gz')), may hold values from -0.29882812 to 0.29882812
- master: float32 [851968], P(('gx', 'gy', 'gz')), may hold values from -6 to 6
- first_moment: float32 [851968], P(('gx', 'gy', 'gz')), may hold values from -3 to 3
- second_moment: float32 [851968], P(('gx', 'gy', 'gz')), may hold values from 0.01 to 1
- step_count: int32 [1], replicated, may hold values from 1 to 7
- step_size: float32 [1], replicated, may hold values from 0.01 to 0.1
Outputs:
- new_master: float32 [851968], P(('gx', 'gy', 'gz'))
- new_first: float32 [851968], P(('gx', 'gy', 'gz'))
- new_second: float32 [851968], P(('gx', 'gy', 'gz'))
- weights: bfloat16 [851968], replicated
The draws below stay inside these ranges and needn't reach their ends.
All inputs are finite; a program needn't handle non-finite values.
Results may differ from the reference program's by a relative error of at most 0.009.
Values may be sent and summed in bfloat16 or wider, within the bound.
No kernel may reach another device: no remote copies, remote signals or barrier semaphores. Data moves between devices by JAX's collectives and lax.ppermute only.
A program may use at most 64 MiB of HBM per device.

```python
import math
import jax
import jax.numpy as jnp
from jax import lax

E = 851968
DEVICES = 32


def strengthened(array, stream_key, source, target, shards_of, factor):
    def block_of(dim):
        return (jnp.arange(array.shape[dim]) // (array.shape[dim] // shards_of)).reshape((-1,) + (1,) * (array.ndim - 1 - dim))

    one_side = jax.random.permutation(stream_key, shards_of)[block_of(target)]
    second = (block_of(target) + shards_of // 2) % shards_of
    return jnp.where((block_of(source) == one_side) | (block_of(source) == second), factor * array, array)


def block_scale(rng, dims, pieces, low, high):
    level, own = 1.0, jax.random.fold_in(rng, 6)
    for axis_at, parts in pieces:
        draws = jnp.exp(jax.random.uniform(jax.random.fold_in(own, axis_at), (parts,), jnp.float32, low / len(pieces), high / len(pieces)))
        level = level * jnp.repeat(draws, dims[axis_at] // parts).reshape([-1 if axis == axis_at else 1 for axis in range(len(dims))])
    return level


def normal_values(stream_key, extent, deviation, reach, pieces=(), kind=jnp.bfloat16):
    values = deviation * jax.random.normal(stream_key, extent, jnp.float32)
    if pieces:
        values = values * block_scale(stream_key, extent, pieces, -0.22, 0.18)
    return jnp.clip(values, -reach, reach).astype(kind)


def noise_with(stream_key, extent, width, limit, shards, heavy, held_as=jnp.bfloat16):
    entries = width * jax.random.normal(stream_key, extent, jnp.float32)
    if shards:
        entries = entries * block_scale(stream_key, extent, shards, -0.22, 0.18)
    return jnp.clip(strengthened(entries, jax.random.fold_in(stream_key, 3), *heavy), -limit, limit).astype(held_as)


def setup_inputs(seed: int = 0) -> dict:
    splits = jax.random.split(jax.random.key(seed), 7)
    gradients = noise_with(splits[0], (DEVICES, E), 0.05, 0.29882812, ((0, 32),), (0, 1, 32, 2.75))
    master = normal_values(splits[1], (E,), 1.0, 6.0, ((0, 32),), jnp.float32)
    first_moment = normal_values(splits[2], (E,), 0.5, 3.0, ((0, 32),), jnp.float32)
    second_moment = jnp.clip(jnp.exp(math.log(1.0) - 4.6051702 * jax.random.uniform(splits[3], (E,), jnp.float32) ** block_scale(splits[3], (E,), ((0, 32),), -0.2, 0.2)), 0.01, 1.0)
    step_count = jax.random.randint(splits[4], (1,), 1, 8).astype(jnp.int32)
    step_size = jnp.clip(jnp.exp(jax.random.uniform(splits[5], (1,), jnp.float32, math.log(0.01), math.log(0.1))), 0.01, 0.1)
    return {"gradients": gradients, "master": master, "first_moment": first_moment, "second_moment": second_moment, "step_count": step_count, "step_size": step_size}


BETA_ONE = 0.9
BETA_TWO = 0.95
EPSILON = 1e-08

def adam_update(summed, master, first_moment, second_moment, step_count, step_size):
    counted = step_count[0].astype(jnp.float32)
    first_fix = 1.0 - jnp.power(jnp.float32(BETA_ONE), counted)
    second_fix = 1.0 - jnp.power(jnp.float32(BETA_TWO), counted)
    new_first = BETA_ONE * first_moment + (1.0 - BETA_ONE) * summed
    new_second = BETA_TWO * second_moment + (1.0 - BETA_TWO) * summed * summed
    update = new_first / first_fix / (jnp.sqrt(new_second / second_fix) + EPSILON)
    new_master = master - step_size[0] * update
    return (new_master, new_first, new_second)

def reference(gradients, master, first_moment, second_moment, step_count, step_size):
    summed = lax.optimization_barrier(jnp.sum(gradients, axis=0, dtype=jnp.float32))
    new_master, new_first, new_second = adam_update(summed, master, first_moment, second_moment, step_count, step_size)
    return (new_master, new_first, new_second, new_master.astype(jnp.bfloat16))
```

```python
import itertools

import jax
import jax.numpy as jnp
from jax import lax
from jax.experimental import pallas as pl
from jax.experimental.pallas import tpu as pltpu
from jax.sharding import PartitionSpec as P


BETA_ONE = 0.9
BETA_TWO = 0.95
EPSILON = 1e-08
LANES = 128
VMEM_LIMIT = 8 << 20
FIRST = 2
X, PAIR, HIGH, LOW = range(4)
SUM_STAGES = ((X, PAIR, LOW), (HIGH,))
SPREAD_STAGES = ((HIGH, LOW), (X, PAIR))


def adam_update(summed, master, first_moment, second_moment, step_count, step_size):
    counted = step_count[0].astype(jnp.float32)
    first_fix = 1.0 - jnp.power(jnp.float32(BETA_ONE), counted)
    second_fix = 1.0 - jnp.power(jnp.float32(BETA_TWO), counted)
    new_first = BETA_ONE * first_moment + (1.0 - BETA_ONE) * summed
    new_second = BETA_TWO * second_moment + (1.0 - BETA_TWO) * summed * summed
    update = new_first / first_fix / (jnp.sqrt(new_second / second_fix) + EPSILON)
    new_master = master - step_size[0] * update
    return (new_master, new_first, new_second)


class Places:
    def __init__(self):
        self.x, self.y, self.z = (lax.axis_size(a) for a in ("gx", "gy", "gz"))
        self.sizes = (self.x, self.y // 2, self.z // 2, 2)

    def offsets(self, digits):
        every = itertools.product(*(range(n if i in digits else 1) for i, n in enumerate(self.sizes)))
        return sorted(every, key=lambda o: (not any(o), sum(v > 0 for v in o)))

    def block(self, sign, offset, other):
        at_x, at_y, at_z = (lax.axis_index(a) for a in ("gx", "gy", "gz"))
        place = (at_x, lax.div(at_y, 2), lax.div(at_z, 2), lax.rem(at_z, 2))
        x, pair, high, low = (
            lax.rem(at + n + sign * o, n) if o else at for at, n, o in zip(place, self.sizes, offset)
        )
        side = lax.rem(at_y, 2)
        side = 1 - side if other else side
        return ((x * self.sizes[1] + pair) * 2 + side) * self.z + high * 2 + low

    def send(self, value, offset):
        moves = []
        for x, pair, side, high, low in itertools.product(
            *(range(n) for n in (*self.sizes[:2], 2, *self.sizes[2:]))
        ):
            to = [(v + o) % n for v, o, n in zip((x, pair, high, low), offset, self.sizes)]
            source, target = (
                ((p[0] * self.sizes[1] + p[1]) * 2 + side) * self.z + p[2] * 2 + p[3]
                for p in ((x, pair, high, low), to)
            )
            moves.append((source, target))
        return lax.ppermute(value, ("gx", "gy", "gz"), moves)

    def swap(self, value):
        return lax.ppermute(value, "gy", [(y, y ^ 1) for y in range(self.y)])


def both(one, two):
    return tuple(a + b for a, b in zip(one, two))


def dense_blocks(gradients, offsets, block, places, after):
    rows = block // LANES
    total = len(offsets) * rows

    def kernel(g_ref, *refs):
        keep_ref, send_ref = refs[len(after) :]
        for other, out_ref in ((True, send_ref), (False, keep_ref)):
            for slot, offset in enumerate(offsets):
                start = pl.multiple_of(places.block(1, offset, other) * block, LANES)
                out_ref[slot * rows : (slot + 1) * rows, :] = g_ref[0, pl.ds(start, block)].reshape(rows, LANES)

    out = jax.ShapeDtypeStruct((total, LANES), gradients.dtype)
    return pl.pallas_call(
        kernel,
        in_specs=[pl.BlockSpec(memory_space=pltpu.VMEM)] + [pl.BlockSpec(memory_space=pl.ANY)] * len(after),
        out_specs=[pl.BlockSpec(memory_space=pltpu.VMEM)] * 2,
        out_shape=[out, out],
        compiler_params=pltpu.CompilerParams(vmem_limit_bytes=VMEM_LIMIT),
        cost_estimate=pl.CostEstimate(
            flops=8 * total * LANES, bytes_accessed=12 * total * LANES, transcendentals=0
        ),
    )(gradients, *after)


def place_blocks(pieces, held, block, total, places):
    rows = block // LANES
    if rows % 8:
        where = jnp.stack([places.block(-1, *one) for one in held])
        found = jnp.concatenate(pieces).reshape(-1, block)
        return jnp.zeros_like(found).at[where].set(found).reshape(-1, LANES)

    def kernel(*refs):
        sources, out_ref, sems = refs[: len(pieces)], refs[len(pieces)], refs[len(pieces) + 1]
        copies = []
        for source in sources:
            for k in range(source.shape[0] // rows):
                at = len(copies)
                start = pl.multiple_of(places.block(-1, *held[at]) * rows, 8)
                copies.append(
                    pltpu.make_async_copy(
                        source.at[pl.ds(k * rows, rows)], out_ref.at[pl.ds(start, rows)], sems.at[at]
                    )
                )
        for copy in copies:
            copy.start()
        for copy in copies:
            copy.wait()

    return pl.pallas_call(
        kernel,
        in_specs=[pl.BlockSpec(memory_space=pl.ANY)] * len(pieces),
        out_specs=pl.BlockSpec(memory_space=pl.ANY),
        out_shape=jax.ShapeDtypeStruct((total // LANES, LANES), pieces[0].dtype),
        scratch_shapes=[pltpu.SemaphoreType.DMA((len(held),))],
        compiler_params=pltpu.CompilerParams(vmem_limit_bytes=VMEM_LIMIT),
        cost_estimate=pl.CostEstimate(flops=total, bytes_accessed=4 * total, transcendentals=0),
    )(*pieces)


def per_device(gradients, master, first_moment, second_moment, step_count, step_size):
    places = Places()
    owned = master.shape[0]
    rows = owned // LANES
    wide, narrow = jnp.float32, gradients.dtype

    near, far = (places.offsets(digits) for digits in SUM_STAGES)
    size = len(far) * rows
    arrived, after = [], []
    for part in (near[:FIRST], near[FIRST:]):
        keep, send = dense_blocks(gradients, [both(o, f) for o in part for f in far], owned, places, after)
        after = [send]
        got = places.swap(send)
        for slot, offset in enumerate(part):
            span = slice(slot * size, (slot + 1) * size)
            value = keep[span].astype(wide) + got[span].astype(wide)
            if any(offset):
                arrived.append(places.send(value.astype(narrow), offset))
            else:
                total = value
    for part in arrived:
        total = total + part.astype(wide)
    moved = []
    for slot, offset in enumerate(far[:-1]):
        moved.append(places.send(total[slot * rows : (slot + 1) * rows].astype(narrow), offset))
    summed = total[-rows:]
    for part in moved:
        summed = summed + part.astype(wide)

    new_master, new_first, new_second = adam_update(
        summed.reshape(owned), master, first_moment, second_moment, step_count, step_size
    )

    far, near = (places.offsets(digits) for digits in SPREAD_STAGES)
    line = [new_master.astype(narrow).reshape(rows, LANES)] * len(far)
    for slot, offset in enumerate(far[:-1]):
        line[slot] = places.send(line[-1], offset)
    line = jnp.concatenate(line, axis=0)
    pieces = [line] * len(near)
    for slot, offset in enumerate(near[:-1]):
        pieces[slot] = places.send(line, offset)
    pieces = pieces + [places.swap(piece) for piece in pieces]
    held = [(both(o, f), other) for other in (False, True) for o in near for f in far]
    weights = place_blocks(pieces, held, owned, gradients.shape[1], places)
    return (new_master, new_first, new_second, weights.reshape(-1))


def solution(mesh):
    in_specs = (
        P(("gx", "gy", "gz"), None),
        P(("gx", "gy", "gz")),
        P(("gx", "gy", "gz")),
        P(("gx", "gy", "gz")),
        P(),
        P(),
    )
    out_specs = (P(("gx", "gy", "gz")), P(("gx", "gy", "gz")), P(("gx", "gy", "gz")), P())

    return jax.shard_map(per_device, mesh=mesh, in_specs=in_specs, out_specs=out_specs, check_vma=False)
```

```python
import itertools

import jax
import jax.numpy as jnp
from jax import lax
from jax.experimental import pallas as pl
from jax.experimental.pallas import tpu as pltpu
from jax.sharding import PartitionSpec as P


BETA_ONE = 0.9
BETA_TWO = 0.95
EPSILON = 1e-08
LANES = 128
VMEM_LIMIT = 8 << 20
X, PAIR, HIGH, LOW = range(4)


def adam_update(summed, master, first_moment, second_moment, step_count, step_size):
    counted = step_count[0].astype(jnp.float32)
    first_fix = 1.0 - jnp.power(jnp.float32(BETA_ONE), counted)
    second_fix = 1.0 - jnp.power(jnp.float32(BETA_TWO), counted)
    new_first = BETA_ONE * first_moment + (1.0 - BETA_ONE) * summed
    new_second = BETA_TWO * second_moment + (1.0 - BETA_TWO) * summed * summed
    update = new_first / first_fix / (jnp.sqrt(new_second / second_fix) + EPSILON)
    new_master = master - step_size[0] * update
    return (new_master, new_first, new_second)


class Places:
    def __init__(self):
        self.x, self.y, self.z = (lax.axis_size(a) for a in ("gx", "gy", "gz"))
        self.sizes = (self.x, self.y // 2, self.z // 2, 2)
        self.square = self.sizes[:2] == (2, 2)

    def offsets(self, digits):
        every = itertools.product(*(range(n if i in digits else 1) for i, n in enumerate(self.sizes)))
        return sorted(every, key=lambda o: (not any(o), sum(v > 0 for v in o)))

    def digits(self, offset, side):
        if not self.square:
            return offset
        one, two = offset[:2]
        return (two + side * (one - two), one + side * (two - one), *offset[2:])

    def block(self, sign, offset, other):
        at_x, at_y, at_z = (lax.axis_index(a) for a in ("gx", "gy", "gz"))
        side = lax.rem(at_y, 2)
        side = 1 - side if other else side
        place = (at_x, lax.div(at_y, 2), lax.div(at_z, 2), lax.rem(at_z, 2))
        x, pair, high, low = (
            lax.rem(at + n + sign * o, n) for at, n, o in zip(place, self.sizes, self.digits(offset, side))
        )
        return ((x * self.sizes[1] + pair) * 2 + side) * self.z + high * 2 + low

    def send(self, value, offset):
        moves = []
        for x, pair, side, high, low in itertools.product(
            *(range(n) for n in (*self.sizes[:2], 2, *self.sizes[2:]))
        ):
            to = [(v + o) % n for v, o, n in zip((x, pair, high, low), self.digits(offset, side), self.sizes)]
            source, target = (
                ((p[0] * self.sizes[1] + p[1]) * 2 + side) * self.z + p[2] * 2 + p[3]
                for p in ((x, pair, high, low), to)
            )
            moves.append((source, target))
        return lax.ppermute(value, ("gx", "gy", "gz"), moves)

    def swap(self, value):
        return lax.ppermute(value, "gy", [(y, y ^ 1) for y in range(self.y)])


def both(one, two):
    return tuple(a + b for a, b in zip(one, two))


def dense_blocks(gradients, offsets, block, places, after):
    rows = block // LANES
    total = len(offsets) * rows

    def kernel(g_ref, *refs):
        keep_ref, send_ref = refs[len(after) :]
        for other, out_ref in ((True, send_ref), (False, keep_ref)):
            for slot, offset in enumerate(offsets):
                start = pl.multiple_of(places.block(1, offset, other) * block, LANES)
                out_ref[slot * rows : (slot + 1) * rows, :] = g_ref[0, pl.ds(start, block)].reshape(rows, LANES)

    out = jax.ShapeDtypeStruct((total, LANES), gradients.dtype)
    return pl.pallas_call(
        kernel,
        in_specs=[pl.BlockSpec(memory_space=pltpu.VMEM)] + [pl.BlockSpec(memory_space=pl.ANY)] * len(after),
        out_specs=[pl.BlockSpec(memory_space=pltpu.VMEM)] * 2,
        out_shape=[out, out],
        compiler_params=pltpu.CompilerParams(vmem_limit_bytes=VMEM_LIMIT),
        cost_estimate=pl.CostEstimate(
            flops=8 * total * LANES, bytes_accessed=12 * total * LANES, transcendentals=0
        ),
    )(gradients, *after)


def place_blocks(pieces, held, block, total, places, into=()):
    rows = block // LANES
    if rows % 8:
        where = jnp.stack([places.block(-1, *one) for one in held])
        found = jnp.concatenate(pieces).reshape(-1, block)
        return jnp.zeros_like(found).at[where].set(found).reshape(-1, LANES)

    def kernel(*refs):
        sources, (out_ref, sems) = refs[: len(pieces)], refs[len(pieces) + len(into) :]
        copies = []
        for source in sources:
            for k in range(source.shape[0] // rows):
                at = len(copies)
                start = pl.multiple_of(places.block(-1, *held[at]) * rows, 8)
                copies.append(
                    pltpu.make_async_copy(
                        source.at[pl.ds(k * rows, rows)], out_ref.at[pl.ds(start, rows)], sems.at[at]
                    )
                )
        for copy in copies:
            copy.start()
        for copy in copies:
            copy.wait()

    return pl.pallas_call(
        kernel,
        in_specs=[pl.BlockSpec(memory_space=pl.ANY)] * (len(pieces) + len(into)),
        out_specs=pl.BlockSpec(memory_space=pl.ANY),
        out_shape=jax.ShapeDtypeStruct((total // LANES, LANES), pieces[0].dtype),
        scratch_shapes=[pltpu.SemaphoreType.DMA((len(held),))],
        input_output_aliases={len(pieces): 0} if into else {},
        compiler_params=pltpu.CompilerParams(vmem_limit_bytes=VMEM_LIMIT),
        cost_estimate=pl.CostEstimate(flops=total, bytes_accessed=4 * total, transcendentals=0),
    )(*pieces, *into)


def per_device(gradients, master, first_moment, second_moment, step_count, step_size):
    places = Places()
    owned = master.shape[0]
    rows = owned // LANES
    wide, narrow = jnp.float32, gradients.dtype

    near, far = places.offsets((X, PAIR)), places.offsets((HIGH, LOW))
    near = near[-2::-1] + near[-1:]
    size = len(far) * rows
    values, after = {}, []
    for part in (near[:1], near[2:3], near[1:2] + near[3:]):
        keep, send = dense_blocks(gradients, [both(o, f) for o in part for f in far], owned, places, after)
        after = [send]
        got = places.swap(send)
        for slot in range(len(part)):
            span = slice(slot * size, (slot + 1) * size)
            values[part[slot]] = keep[span].astype(wide) + got[span].astype(wide)

    def plane_sent(value, offset):
        return places.send(value.astype(narrow), offset).astype(wide)

    total = values[near[-1]]
    if places.square:
        corner, second, first = near[:3]
        passing = plane_sent(values[corner], first)
        total = total + plane_sent(values[first], first)
        total = total + plane_sent(values[second] + passing, second)
    else:
        for offset in near[:-1]:
            total = total + plane_sent(values[offset], offset)
    moved = []
    for slot, offset in enumerate(far[:-1]):
        moved.append(places.send(total[slot * rows : (slot + 1) * rows].astype(narrow), offset))
    summed = total[-rows:]
    for part in moved:
        summed = summed + part.astype(wide)

    state = (summed.reshape(owned), master, first_moment, second_moment, step_count, step_size)
    block = adam_update(*state)[0].astype(narrow).reshape(rows, LANES)
    new_master, new_first, new_second = adam_update(*lax.optimization_barrier(state))

    line = [block] * len(far)
    for slot, offset in enumerate(far[:-1]):
        line[slot] = places.send(line[-1], offset)
    line = jnp.concatenate(line, axis=0)

    def plane_spread(value, offset):
        return places.send(value, offset)

    near = near[-2::-1] + near[-1:]
    pieces = [plane_spread(line, offset) for offset in near[:-1]] + [line]
    swapped = []
    for piece in pieces:
        swapped.append(places.swap(piece))
    held = [(both(o, f), other) for other in (False, True) for o in near for f in far]
    weights = ()
    for part in (pieces, swapped) if rows % 8 == 0 else (pieces + swapped,):
        weights = [place_blocks(part, held[: len(part) * len(far)], owned, gradients.shape[1], places, weights)]
        held = held[len(part) * len(far) :]
    return (new_master, new_first, new_second, weights[0].reshape(-1))


def solution(mesh):
    in_specs = (
        P(("gx", "gy", "gz"), None),
        P(("gx", "gy", "gz")),
        P(("gx", "gy", "gz")),
        P(("gx", "gy", "gz")),
        P(),
        P(),
    )
    out_specs = (P(("gx", "gy", "gz")), P(("gx", "gy", "gz")), P(("gx", "gy", "gz")), P())

    return jax.shard_map(per_device, mesh=mesh, in_specs=in_specs, out_specs=out_specs, check_vma=False)
```

```python
import itertools

import jax
import jax.numpy as jnp
from jax import lax
from jax.experimental import pallas as pl
from jax.experimental.pallas import tpu as pltpu
from jax.sharding import PartitionSpec as P


BETA_ONE = 0.9
BETA_TWO = 0.95
EPSILON = 1e-08
LANES = 128
VMEM_LIMIT = 8 << 20
X, PAIR, HIGH, LOW = range(4)


def adam_update(summed, master, first_moment, second_moment, step_count, step_size):
    counted = step_count[0].astype(jnp.float32)
    first_fix = 1.0 - jnp.power(jnp.float32(BETA_ONE), counted)
    second_fix = 1.0 - jnp.power(jnp.float32(BETA_TWO), counted)
    new_first = BETA_ONE * first_moment + (1.0 - BETA_ONE) * summed
    new_second = BETA_TWO * second_moment + (1.0 - BETA_TWO) * summed * summed
    update = new_first / first_fix / (jnp.sqrt(new_second / second_fix) + EPSILON)
    new_master = master - step_size[0] * update
    return (new_master, new_first, new_second)


class Places:
    def __init__(self):
        self.x, self.y, self.z = (lax.axis_size(a) for a in ("gx", "gy", "gz"))
        self.sizes = (self.x, self.y // 2, self.z // 2, 2)
        self.square = self.sizes[:2] == (2, 2)

    def offsets(self, digits):
        every = itertools.product(*(range(n if i in digits else 1) for i, n in enumerate(self.sizes)))
        return sorted(every, key=lambda o: (not any(o), sum(v > 0 for v in o)))

    def digits(self, offset, side):
        if not self.square:
            return offset
        one, two = offset[:2]
        return (two + side * (one - two), one + side * (two - one), *offset[2:])

    def block(self, sign, offset, other):
        at_x, at_y, at_z = (lax.axis_index(a) for a in ("gx", "gy", "gz"))
        side = lax.rem(at_y, 2)
        side = 1 - side if other else side
        place = (at_x, lax.div(at_y, 2), lax.div(at_z, 2), lax.rem(at_z, 2))
        x, pair, high, low = (
            lax.rem(at + n + sign * o, n) for at, n, o in zip(place, self.sizes, self.digits(offset, side))
        )
        return ((x * self.sizes[1] + pair) * 2 + side) * self.z + high * 2 + low

    def send(self, value, offset):
        moves = []
        for x, pair, side, high, low in itertools.product(
            *(range(n) for n in (*self.sizes[:2], 2, *self.sizes[2:]))
        ):
            to = [(v + o) % n for v, o, n in zip((x, pair, high, low), self.digits(offset, side), self.sizes)]
            source, target = (
                ((p[0] * self.sizes[1] + p[1]) * 2 + side) * self.z + p[2] * 2 + p[3]
                for p in ((x, pair, high, low), to)
            )
            moves.append((source, target))
        return lax.ppermute(value, ("gx", "gy", "gz"), moves)

    def swap(self, value):
        return lax.ppermute(value, "gy", [(y, y ^ 1) for y in range(self.y)])


def both(one, two):
    return tuple(a + b for a, b in zip(one, two))


def dense_blocks(gradients, offsets, block, places, after):
    rows = block // LANES
    total = len(offsets) * rows

    def kernel(g_ref, *refs):
        keep_ref, send_ref = refs[len(after) :]
        for other, out_ref in ((True, send_ref), (False, keep_ref)):
            for slot, offset in enumerate(offsets):
                start = pl.multiple_of(places.block(1, offset, other) * block, LANES)
                out_ref[slot * rows : (slot + 1) * rows, :] = g_ref[0, pl.ds(start, block)].reshape(rows, LANES)

    out = jax.ShapeDtypeStruct((total, LANES), gradients.dtype)
    return pl.pallas_call(
        kernel,
        in_specs=[pl.BlockSpec(memory_space=pltpu.VMEM)] + [pl.BlockSpec(memory_space=pl.ANY)] * len(after),
        out_specs=[pl.BlockSpec(memory_space=pltpu.VMEM)] * 2,
        out_shape=[out, out],
        compiler_params=pltpu.CompilerParams(vmem_limit_bytes=VMEM_LIMIT),
        cost_estimate=pl.CostEstimate(
            flops=8 * total * LANES, bytes_accessed=12 * total * LANES, transcendentals=0
        ),
    )(gradients, *after)


def place_blocks(pieces, held, block, total, places, into=()):
    rows = block // LANES
    if rows % 8:
        where = jnp.stack([places.block(-1, *one) for one in held])
        found = jnp.concatenate(pieces).reshape(-1, block)
        return jnp.zeros_like(found).at[where].set(found).reshape(-1, LANES)

    def kernel(*refs):
        sources, (out_ref, sems) = refs[: len(pieces)], refs[len(pieces) + len(into) :]
        copies = []
        for source in sources:
            for k in range(source.shape[0] // rows):
                at = len(copies)
                start = pl.multiple_of(places.block(-1, *held[at]) * rows, 8)
                copies.append(
                    pltpu.make_async_copy(
                        source.at[pl.ds(k * rows, rows)], out_ref.at[pl.ds(start, rows)], sems.at[at]
                    )
                )
        for copy in copies:
            copy.start()
        for copy in copies:
            copy.wait()

    return pl.pallas_call(
        kernel,
        in_specs=[pl.BlockSpec(memory_space=pl.ANY)] * (len(pieces) + len(into)),
        out_specs=pl.BlockSpec(memory_space=pl.ANY),
        out_shape=jax.ShapeDtypeStruct((total // LANES, LANES), pieces[0].dtype),
        scratch_shapes=[pltpu.SemaphoreType.DMA((len(held),))],
        input_output_aliases={len(pieces): 0} if into else {},
        compiler_params=pltpu.CompilerParams(vmem_limit_bytes=VMEM_LIMIT),
        cost_estimate=pl.CostEstimate(flops=total, bytes_accessed=4 * total, transcendentals=0),
    )(*pieces, *into)


def per_device(gradients, master, first_moment, second_moment, step_count, step_size):
    places = Places()
    owned = master.shape[0]
    rows = owned // LANES
    wide, narrow = jnp.float32, gradients.dtype

    near, far = places.offsets((X, PAIR)), places.offsets((HIGH, LOW))
    near = near[-2::-1] + near[-1:]
    far = far[1:-1] + far[:1] + far[-1:]
    size = len(far) * rows
    values, after = {}, []
    for part in (near[:1], near[2:3], near[1:2] + near[3:]):
        keep, send = dense_blocks(gradients, [both(o, f) for o in part for f in far], owned, places, after)
        after = [send]
        got = places.swap(send)
        for slot in range(len(part)):
            span = slice(slot * size, (slot + 1) * size)
            values[part[slot]] = keep[span].astype(wide) + got[span].astype(wide)

    def plane_sent(value, offset):
        return places.send(value.astype(narrow), offset).astype(wide)

    total = values[near[-1]]
    if places.square:
        corner, second, first = near[:3]
        passing = plane_sent(values[corner], first)
        direct = plane_sent(values[first], first)
        joined = values[second] + passing
        half = size // 2
        ahead = plane_sent(joined[:half], second)
        behind = plane_sent(joined[half:], second)
        total, direct, ahead = lax.optimization_barrier((total, direct, ahead))
        total = total + direct
        ahead = total[:half] + ahead
    else:
        for offset in near[:-1]:
            total = total + plane_sent(values[offset], offset)
        half = 0
        ahead, behind = total[:0], jnp.zeros_like(total)
    moved = []

    def line_sent(values, offsets):
        for slot, offset in enumerate(offsets):
            part = values[slot * rows : (slot + 1) * rows].astype(narrow)
            moved.append((part, places.send(part, offset)))

    count = half // rows
    line_sent(ahead, far[:count])
    if count:
        *_, total, behind = lax.optimization_barrier((*(part for part, _ in moved), total, behind))
    total = total[half:] + behind
    line_sent(total, far[count:-1])
    moved = [part for _, part in moved]
    summed = total[-rows:]
    for part in moved:
        summed = summed + part.astype(wide)

    state = (summed.reshape(owned), master, first_moment, second_moment, step_count, step_size)
    block = adam_update(*state)[0].astype(narrow).reshape(rows, LANES)
    new_master, new_first, new_second = adam_update(*lax.optimization_barrier(state))

    line = [block] * len(far)
    for slot, offset in enumerate(far[:-1]):
        line[slot] = places.send(line[-1], offset)
    line = jnp.concatenate(line, axis=0)

    def plane_spread(value, offset):
        return places.send(value, offset)

    near = near[-2::-1] + near[-1:]
    pieces = [plane_spread(line, offset) for offset in near[:-1]] + [line]
    swapped = []
    for piece in pieces:
        swapped.append(places.swap(piece))
    held = [[(both(o, f), other) for f in far] for other in (False, True) for o in near]
    pieces += swapped
    last = [len(pieces) - 2] if rows % 8 == 0 else []
    weights = ()
    for part in ([k for k in range(len(pieces)) if k not in last], last):
        if part:
            blocks = sum((held[k] for k in part), [])
            weights = [
                place_blocks([pieces[k] for k in part], blocks, owned, gradients.shape[1], places, weights)
            ]
    return (new_master, new_first, new_second, weights[0].reshape(-1))


def solution(mesh):
    in_specs = (
        P(("gx", "gy", "gz"), None),
        P(("gx", "gy", "gz")),
        P(("gx", "gy", "gz")),
        P(("gx", "gy", "gz")),
        P(),
        P(),
    )
    out_specs = (P(("gx", "gy", "gz")), P(("gx", "gy", "gz")), P(("gx", "gy", "gz")), P())

    return jax.shard_map(per_device, mesh=mesh, in_specs=in_specs, out_specs=out_specs, check_vma=False)
```

```python
import itertools

import jax
import jax.numpy as jnp
from jax import lax
from jax.experimental import pallas as pl
from jax.experimental.pallas import tpu as pltpu
from jax.sharding import PartitionSpec as P


BETA_ONE = 0.9
BETA_TWO = 0.95
EPSILON = 1e-08
LANES = 128
VMEM_LIMIT = 8 << 20
X, PAIR, HIGH, LOW = range(4)


def adam_update(summed, master, first_moment, second_moment, step_count, step_size):
    counted = step_count[0].astype(jnp.float32)
    first_fix = 1.0 - jnp.power(jnp.float32(BETA_ONE), counted)
    second_fix = 1.0 - jnp.power(jnp.float32(BETA_TWO), counted)
    new_first = BETA_ONE * first_moment + (1.0 - BETA_ONE) * summed
    new_second = BETA_TWO * second_moment + (1.0 - BETA_TWO) * summed * summed
    update = new_first / first_fix / (jnp.sqrt(new_second / second_fix) + EPSILON)
    new_master = master - step_size[0] * update
    return (new_master, new_first, new_second)


class Places:
    def __init__(self):
        self.x, self.y, self.z = (lax.axis_size(a) for a in ("gx", "gy", "gz"))
        self.sizes = (self.x, self.y // 2, self.z // 2, 2)
        self.square = self.sizes[:2] == (2, 2)

    def offsets(self, digits):
        every = itertools.product(*(range(n if i in digits else 1) for i, n in enumerate(self.sizes)))
        return sorted(every, key=lambda o: (not any(o), sum(v > 0 for v in o)))

    def digits(self, offset, side):
        if not self.square:
            return offset
        one, two = offset[:2]
        return (two + side * (one - two), one + side * (two - one), *offset[2:])

    def block(self, sign, offset, other):
        at_x, at_y, at_z = (lax.axis_index(a) for a in ("gx", "gy", "gz"))
        side = lax.rem(at_y, 2)
        side = 1 - side if other else side
        place = (at_x, lax.div(at_y, 2), lax.div(at_z, 2), lax.rem(at_z, 2))
        x, pair, high, low = (
            lax.rem(at + n + sign * o, n) for at, n, o in zip(place, self.sizes, self.digits(offset, side))
        )
        return ((x * self.sizes[1] + pair) * 2 + side) * self.z + high * 2 + low

    def send(self, value, offset):
        moves = []
        for x, pair, side, high, low in itertools.product(
            *(range(n) for n in (*self.sizes[:2], 2, *self.sizes[2:]))
        ):
            to = [(v + o) % n for v, o, n in zip((x, pair, high, low), self.digits(offset, side), self.sizes)]
            source, target = (
                ((p[0] * self.sizes[1] + p[1]) * 2 + side) * self.z + p[2] * 2 + p[3]
                for p in ((x, pair, high, low), to)
            )
            moves.append((source, target))
        return lax.ppermute(value, ("gx", "gy", "gz"), moves)

    def swap(self, value):
        return lax.ppermute(value, "gy", [(y, y ^ 1) for y in range(self.y)])


def both(one, two):
    return tuple(a + b for a, b in zip(one, two))


def dense_blocks(gradients, offsets, block, places, after, direct=False):
    rows = block // LANES
    total = len(offsets) * rows

    def fetching(g_ref, keep_ref, send_ref, held, sems):
        copies = []
        for other in (True, False):
            for offset in offsets:
                start = pl.multiple_of(places.block(1, offset, other) * block, LANES)
                at = len(copies)
                copies.append(pltpu.make_async_copy(g_ref.at[:, pl.ds(start, block)], held.at[at], sems.at[at]))
        for copy in copies:
            copy.start()
        for n, copy in enumerate(copies):
            copy.wait()
            out_ref, slot = (send_ref, keep_ref)[n // len(offsets)], n % len(offsets)
            out_ref[slot * rows : (slot + 1) * rows, :] = held[n, 0, :].reshape(rows, LANES)

    def kernel(g_ref, *refs):
        keep_ref, send_ref = refs[len(after) :]
        for other, out_ref in ((True, send_ref), (False, keep_ref)):
            for slot, offset in enumerate(offsets):
                start = pl.multiple_of(places.block(1, offset, other) * block, LANES)
                out_ref[slot * rows : (slot + 1) * rows, :] = g_ref[0, pl.ds(start, block)].reshape(rows, LANES)

    out = jax.ShapeDtypeStruct((total, LANES), gradients.dtype)
    if direct:
        return pl.pallas_call(
            fetching,
            in_specs=[pl.BlockSpec(memory_space=pltpu.HBM)],
            out_specs=[pl.BlockSpec(memory_space=pltpu.VMEM)] * 2,
            out_shape=[out, out],
            scratch_shapes=[
                pltpu.VMEM((2 * len(offsets), 1, block), gradients.dtype),
                pltpu.SemaphoreType.DMA((2 * len(offsets),)),
            ],
            compiler_params=pltpu.CompilerParams(vmem_limit_bytes=VMEM_LIMIT),
            cost_estimate=pl.CostEstimate(
                flops=8 * total * LANES, bytes_accessed=12 * total * LANES, transcendentals=0
            ),
        )(pltpu.with_memory_space_constraint(gradients, pltpu.HBM))
    return pl.pallas_call(
        kernel,
        in_specs=[pl.BlockSpec(memory_space=pltpu.VMEM)] + [pl.BlockSpec(memory_space=pl.ANY)] * len(after),
        out_specs=[pl.BlockSpec(memory_space=pltpu.VMEM)] * 2,
        out_shape=[out, out],
        compiler_params=pltpu.CompilerParams(vmem_limit_bytes=VMEM_LIMIT),
        cost_estimate=pl.CostEstimate(
            flops=8 * total * LANES, bytes_accessed=12 * total * LANES, transcendentals=0
        ),
    )(gradients, *after)


def place_blocks(pieces, held, block, total, places, into=()):
    rows = block // LANES
    if rows % 8:
        where = jnp.stack([places.block(-1, *one) for one in held])
        found = jnp.concatenate(pieces).reshape(-1, block)
        return jnp.zeros_like(found).at[where].set(found).reshape(-1, LANES)

    def kernel(*refs):
        sources, (out_ref, sems) = refs[: len(pieces)], refs[len(pieces) + len(into) :]
        copies = []
        for source in sources:
            for k in range(source.shape[0] // rows):
                at = len(copies)
                start = pl.multiple_of(places.block(-1, *held[at]) * rows, 8)
                copies.append(
                    pltpu.make_async_copy(
                        source.at[pl.ds(k * rows, rows)], out_ref.at[pl.ds(start, rows)], sems.at[at]
                    )
                )
        for copy in copies:
            copy.start()
        for copy in copies:
            copy.wait()

    return pl.pallas_call(
        kernel,
        in_specs=[pl.BlockSpec(memory_space=pl.ANY)] * (len(pieces) + len(into)),
        out_specs=pl.BlockSpec(memory_space=pl.ANY),
        out_shape=jax.ShapeDtypeStruct((total // LANES, LANES), pieces[0].dtype),
        scratch_shapes=[pltpu.SemaphoreType.DMA((len(held),))],
        input_output_aliases={len(pieces): 0} if into else {},
        compiler_params=pltpu.CompilerParams(vmem_limit_bytes=VMEM_LIMIT),
        cost_estimate=pl.CostEstimate(flops=total, bytes_accessed=4 * total, transcendentals=0),
    )(*pieces, *into)


def per_device(gradients, master, first_moment, second_moment, step_count, step_size):
    places = Places()
    owned = master.shape[0]
    rows = owned // LANES
    wide, narrow = jnp.float32, gradients.dtype

    near, far = places.offsets((X, PAIR)), places.offsets((HIGH, LOW))
    near = near[-2::-1] + near[-1:]
    far = far[1:-1] + far[:1] + far[-1:]
    size = len(far) * rows
    values, after = {}, []
    for n, part in enumerate(filter(None, (near[:1], near[2:3], near[1:2] + near[3:]))):
        keep, send = dense_blocks(gradients, [both(o, f) for o in part for f in far], owned, places, after, n == 0)
        after = [send]
        got = places.swap(send)
        for slot in range(len(part)):
            span = slice(slot * size, (slot + 1) * size)
            values[part[slot]] = keep[span].astype(wide) + got[span].astype(wide)

    def plane_sent(value, offset):
        return places.send(value.astype(narrow), offset).astype(wide)

    total = values[near[-1]]
    if places.square:
        corner, second, first = near[:3]
        passing = plane_sent(values[corner], first)
        direct = plane_sent(values[first], first)
        joined = values[second] + passing
        half = size // 2
        ahead = plane_sent(joined[:half], second)
        behind = plane_sent(joined[half:], second)
        total, direct, ahead = lax.optimization_barrier((total, direct, ahead))
        total = total + direct
        ahead = total[:half] + ahead
    else:
        for offset in near[:-1]:
            total = total + plane_sent(values[offset], offset)
        half = 0
        ahead, behind = total[:0], jnp.zeros_like(total)
    moved = []

    def line_sent(values, offsets):
        for slot, offset in enumerate(offsets):
            part = values[slot * rows : (slot + 1) * rows].astype(narrow)
            moved.append((part, places.send(part, offset)))

    count = half // rows
    line_sent(ahead, far[:count])
    if count:
        *_, total, behind = lax.optimization_barrier((*(part for part, _ in moved), total, behind))
    total = total[half:] + behind
    line_sent(total, far[count:-1])
    moved = [part for _, part in moved]
    summed = total[-rows:]
    for part in moved:
        summed = summed + part.astype(wide)

    state = (summed.reshape(owned), master, first_moment, second_moment, step_count, step_size)
    block = adam_update(*state)[0].astype(narrow).reshape(rows, LANES)
    new_master, new_first, new_second = adam_update(*lax.optimization_barrier(state))

    line = [block] * len(far)
    for slot, offset in enumerate(far[:-1]):
        line[slot] = places.send(line[-1], offset)
    line = jnp.concatenate(line, axis=0)

    def plane_spread(value, offset):
        return places.send(value, offset)

    near = near[-2::-1] + near[-1:]
    pieces = [plane_spread(line, offset) for offset in near[:-1]] + [line]
    swapped = []
    for piece in pieces:
        swapped.append(places.swap(piece))
    held = [[(both(o, f), other) for f in far] for other in (False, True) for o in near]
    pieces += swapped
    last = [len(pieces) - 2] if rows % 8 == 0 else []
    weights = ()
    for part in ([k for k in range(len(pieces)) if k not in last], last):
        if part:
            blocks = sum((held[k] for k in part), [])
            weights = [
                place_blocks([pieces[k] for k in part], blocks, owned, gradients.shape[1], places, weights)
            ]
    return (new_master, new_first, new_second, weights[0].reshape(-1))


def solution(mesh):
    in_specs = (
        P(("gx", "gy", "gz"), None),
        P(("gx", "gy", "gz")),
        P(("gx", "gy", "gz")),
        P(("gx", "gy", "gz")),
        P(),
        P(),
    )
    out_specs = (P(("gx", "gy", "gz")), P(("gx", "gy", "gz")), P(("gx", "gy", "gz")), P())

    return jax.shard_map(per_device, mesh=mesh, in_specs=in_specs, out_specs=out_specs, check_vma=False)
```

```python
import itertools

import jax
import jax.numpy as jnp
from jax import lax
from jax.experimental import pallas as pl
from jax.experimental.pallas import tpu as pltpu
from jax.sharding import PartitionSpec as P


BETA_ONE = 0.9
BETA_TWO = 0.95
EPSILON = 1e-08
LANES = 128
VMEM_LIMIT = 8 << 20
X, PAIR, HIGH, LOW = range(4)


def adam_update(summed, master, first_moment, second_moment, step_count, step_size):
    counted = step_count[0].astype(jnp.float32)
    first_fix = 1.0 - jnp.power(jnp.float32(BETA_ONE), counted)
    second_fix = 1.0 - jnp.power(jnp.float32(BETA_TWO), counted)
    new_first = BETA_ONE * first_moment + (1.0 - BETA_ONE) * summed
    new_second = BETA_TWO * second_moment + (1.0 - BETA_TWO) * summed * summed
    update = new_first / first_fix / (jnp.sqrt(new_second / second_fix) + EPSILON)
    new_master = master - step_size[0] * update
    return (new_master, new_first, new_second)


class Places:
    def __init__(self):
        self.x, self.y, self.z = (lax.axis_size(a) for a in ("gx", "gy", "gz"))
        self.sizes = (self.x, self.y // 2, self.z // 2, 2)
        self.square = self.sizes[:2] == (2, 2)

    def offsets(self, digits):
        every = itertools.product(*(range(n if i in digits else 1) for i, n in enumerate(self.sizes)))
        return sorted(every, key=lambda o: (not any(o), sum(v > 0 for v in o)))

    def digits(self, offset, side):
        if not self.square:
            return offset
        one, two = offset[:2]
        return (two + side * (one - two), one + side * (two - one), *offset[2:])

    def block(self, sign, offset, other):
        at_x, at_y, at_z = (lax.axis_index(a) for a in ("gx", "gy", "gz"))
        side = lax.rem(at_y, 2)
        side = 1 - side if other else side
        place = (at_x, lax.div(at_y, 2), lax.div(at_z, 2), lax.rem(at_z, 2))
        x, pair, high, low = (
            lax.rem(at + n + sign * o, n) for at, n, o in zip(place, self.sizes, self.digits(offset, side))
        )
        return ((x * self.sizes[1] + pair) * 2 + side) * self.z + high * 2 + low

    def send(self, value, offset):
        moves = []
        for x, pair, side, high, low in itertools.product(
            *(range(n) for n in (*self.sizes[:2], 2, *self.sizes[2:]))
        ):
            to = [(v + o) % n for v, o, n in zip((x, pair, high, low), self.digits(offset, side), self.sizes)]
            source, target = (
                ((p[0] * self.sizes[1] + p[1]) * 2 + side) * self.z + p[2] * 2 + p[3]
                for p in ((x, pair, high, low), to)
            )
            moves.append((source, target))
        return lax.ppermute(value, ("gx", "gy", "gz"), moves)

    def swap(self, value):
        return lax.ppermute(value, "gy", [(y, y ^ 1) for y in range(self.y)])


def both(one, two):
    return tuple(a + b for a, b in zip(one, two))


def dense_blocks(gradients, offsets, block, places, after, direct=False):
    rows = block // LANES
    total = len(offsets) * rows

    def fetching(g_ref, send_ref, held, sems):
        copies = []
        for at, offset in enumerate(offsets):
            start = pl.multiple_of(places.block(1, offset, True) * block, LANES)
            copies.append(pltpu.make_async_copy(g_ref.at[:, pl.ds(start, block)], held.at[at], sems.at[at]))
        for copy in copies:
            copy.start()
        for n, copy in enumerate(copies):
            copy.wait()
            send_ref[n * rows : (n + 1) * rows, :] = held[n, 0, :].reshape(rows, LANES)

    def kernel(g_ref, *refs):
        outs = refs[len(after) :]
        for other, out_ref in zip((False, True), outs):
            for slot, offset in enumerate(offsets):
                start = pl.multiple_of(places.block(1, offset, other) * block, LANES)
                out_ref[slot * rows : (slot + 1) * rows, :] = g_ref[0, pl.ds(start, block)].reshape(rows, LANES)

    out = jax.ShapeDtypeStruct((total, LANES), gradients.dtype)
    if direct:
        send = pl.pallas_call(
            fetching,
            in_specs=[pl.BlockSpec(memory_space=pltpu.HBM)],
            out_specs=pl.BlockSpec(memory_space=pltpu.VMEM),
            out_shape=out,
            scratch_shapes=[
                pltpu.VMEM((len(offsets), 1, block), gradients.dtype),
                pltpu.SemaphoreType.DMA((len(offsets),)),
            ],
            compiler_params=pltpu.CompilerParams(vmem_limit_bytes=VMEM_LIMIT),
            cost_estimate=pl.CostEstimate(
                flops=4 * total * LANES, bytes_accessed=6 * total * LANES, transcendentals=0
            ),
        )(pltpu.with_memory_space_constraint(gradients, pltpu.HBM))
        after = [send]
    sides = 1 if direct else 2
    made = pl.pallas_call(
        kernel,
        in_specs=[pl.BlockSpec(memory_space=pltpu.VMEM)] + [pl.BlockSpec(memory_space=pl.ANY)] * len(after),
        out_specs=[pl.BlockSpec(memory_space=pltpu.VMEM)] * sides,
        out_shape=[out] * sides,
        compiler_params=pltpu.CompilerParams(vmem_limit_bytes=VMEM_LIMIT),
        cost_estimate=pl.CostEstimate(
            flops=8 * total * LANES, bytes_accessed=12 * total * LANES, transcendentals=0
        ),
    )(gradients, *after)
    return (*made, send) if direct else made


def place_blocks(pieces, held, block, total, places, into=()):
    rows = block // LANES
    if rows % 8:
        where = jnp.stack([places.block(-1, *one) for one in held])
        found = jnp.concatenate(pieces).reshape(-1, block)
        return jnp.zeros_like(found).at[where].set(found).reshape(-1, LANES)

    def kernel(*refs):
        sources, (out_ref, sems) = refs[: len(pieces)], refs[len(pieces) + len(into) :]
        copies = []
        for source in sources:
            for k in range(source.shape[0] // rows):
                at = len(copies)
                start = pl.multiple_of(places.block(-1, *held[at]) * rows, 8)
                copies.append(
                    pltpu.make_async_copy(
                        source.at[pl.ds(k * rows, rows)], out_ref.at[pl.ds(start, rows)], sems.at[at]
                    )
                )
        for copy in copies:
            copy.start()
        for copy in copies:
            copy.wait()

    return pl.pallas_call(
        kernel,
        in_specs=[pl.BlockSpec(memory_space=pl.ANY)] * (len(pieces) + len(into)),
        out_specs=pl.BlockSpec(memory_space=pl.ANY),
        out_shape=jax.ShapeDtypeStruct((total // LANES, LANES), pieces[0].dtype),
        scratch_shapes=[pltpu.SemaphoreType.DMA((len(held),))],
        input_output_aliases={len(pieces): 0} if into else {},
        compiler_params=pltpu.CompilerParams(vmem_limit_bytes=VMEM_LIMIT),
        cost_estimate=pl.CostEstimate(flops=total, bytes_accessed=4 * total, transcendentals=0),
    )(*pieces, *into)


def per_device(gradients, master, first_moment, second_moment, step_count, step_size):
    places = Places()
    owned = master.shape[0]
    rows = owned // LANES
    wide, narrow = jnp.float32, gradients.dtype

    near, far = places.offsets((X, PAIR)), places.offsets((HIGH, LOW))
    near = near[-2::-1] + near[-1:]
    far = far[1:-1] + far[:1] + far[-1:]
    size = len(far) * rows
    values, after = {}, []
    for n, part in enumerate(filter(None, (near[:1], near[2:3], near[1:2] + near[3:]))):
        keep, send = dense_blocks(gradients, [both(o, f) for o in part for f in far], owned, places, after, n == 0)
        after = [send]
        got = places.swap(send)
        for slot in range(len(part)):
            span = slice(slot * size, (slot + 1) * size)
            values[part[slot]] = keep[span].astype(wide) + got[span].astype(wide)

    def plane_sent(value, offset):
        return places.send(value.astype(narrow), offset).astype(wide)

    total = values[near[-1]]
    if places.square:
        corner, second, first = near[:3]
        passing = plane_sent(values[corner], first)
        direct = plane_sent(values[first], first)
        joined = values[second] + passing
        half = size // 2
        ahead = plane_sent(joined[:half], second)
        behind = plane_sent(joined[half:], second)
        total, direct, ahead = lax.optimization_barrier((total, direct, ahead))
        total = total + direct
        ahead = total[:half] + ahead
    else:
        for offset in near[:-1]:
            total = total + plane_sent(values[offset], offset)
        half = 0
        ahead, behind = total[:0], jnp.zeros_like(total)
    moved = []

    def line_sent(values, offsets):
        for slot, offset in enumerate(offsets):
            part = values[slot * rows : (slot + 1) * rows].astype(narrow)
            moved.append((part, places.send(part, offset)))

    count = half // rows
    line_sent(ahead, far[:count])
    if count:
        *_, total, behind = lax.optimization_barrier((*(part for part, _ in moved), total, behind))
    total = total[half:] + behind
    line_sent(total, far[count:-1])
    moved = [part for _, part in moved]
    summed = total[-rows:]
    for part in moved:
        summed = summed + part.astype(wide)

    state = (summed.reshape(owned), master, first_moment, second_moment, step_count, step_size)
    block = adam_update(*state)[0].astype(narrow).reshape(rows, LANES)
    new_master, new_first, new_second = adam_update(*lax.optimization_barrier(state))

    line = [block] * len(far)
    for slot, offset in enumerate(far[:-1]):
        line[slot] = places.send(line[-1], offset)
    line = jnp.concatenate(line, axis=0)

    def plane_spread(value, offset):
        return places.send(value, offset)

    near = near[-2::-1] + near[-1:]
    pieces = [plane_spread(line, offset) for offset in near[:-1]] + [line]
    swapped = []
    for piece in pieces:
        swapped.append(places.swap(piece))
    held = [[(both(o, f), other) for f in far] for other in (False, True) for o in near]
    pieces += swapped
    last = [len(pieces) - 2] if rows % 8 == 0 else []
    weights = ()
    for part in ([k for k in range(len(pieces)) if k not in last], last):
        if part:
            blocks = sum((held[k] for k in part), [])
            weights = [
                place_blocks([pieces[k] for k in part], blocks, owned, gradients.shape[1], places, weights)
            ]
    return (new_master, new_first, new_second, weights[0].reshape(-1))


def solution(mesh):
    in_specs = (
        P(("gx", "gy", "gz"), None),
        P(("gx", "gy", "gz")),
        P(("gx", "gy", "gz")),
        P(("gx", "gy", "gz")),
        P(),
        P(),
    )
    out_specs = (P(("gx", "gy", "gz")), P(("gx", "gy", "gz")), P(("gx", "gy", "gz")), P())

    return jax.shard_map(per_device, mesh=mesh, in_specs=in_specs, out_specs=out_specs, check_vma=False)
```
